16 devices in a mesh: dp: 2 (over y, z), tp: 8 (over x, core).
Axes of the slice: x: 4, y: 2, z: 1, core: 2. Of those that a mesh axis runs over, the one named last changes fastest.
The devices are a block of a 4x4x8 slice.
Arguments:
- hidden: bfloat16 [6, 1536, 2048], P('dp', 'tp'), parts along dimension 0
- grad_out: bfloat16 [6, 1536, 2048], P('dp', 'tp'), parts along dimension 0
- prefix_len: int32 [6], P('dp'), parts along dimension 0
- valid_len: int32 [6], P('dp'), parts along dimension 0
- attn_norm: bfloat16 [2048], replicated
- w_query: bfloat16 [2048, 2048], P(None, 'tp')
- w_key: bfloat16 [2048, 256], replicated
- w_value: bfloat16 [2048, 256], replicated
- w_out: bfloat16 [2048, 2048], P('tp')
- mlp_norm: bfloat16 [2048], replicated
- w_gate: bfloat16 [2048, 16384], P(None, 'tp')
- w_up: bfloat16 [2048, 16384], P(None, 'tp')
- w_down: bfloat16 [16384, 2048], P('tp')
Outputs:
- output 1: bfloat16 [6, 1536, 2048], P('dp', 'tp'), parts along dimension 0
- output 2: bfloat16 [6, 1536, 2048], P('dp', 'tp'), parts along dimension 0
- output 3: float32 [4096], P('dp'), parts along dimension 0
- output 4: float32 [4096, 2048], P('dp', 'tp'), parts along dimension 0
- output 5: float32 [4096, 256], P('dp'), parts along dimension 0
- output 6: float32 [4096, 256], P('dp'), parts along dimension 0
- output 7: float32 [4096, 2048], P(('dp', 'tp')), parts along dimension 0
- output 8: float32 [4096], P('dp'), parts along dimension 0
- output 9: float32 [4096, 16384], P('dp', 'tp'), parts along dimension 0
- output 10: float32 [4096, 16384], P('dp', 'tp'), parts along dimension 0
- output 11: float32 [32768, 2048], P(('dp', 'tp')), parts along dimension 0
There are 2 independent parts. The reference program is written for one: setup_inputs(seed, part) draws one part's arguments, and reference() takes and returns one part's arrays. A program takes and returns all parts, laid end to end along the dimension named above; an argument that names none is the same for every part.
All inputs are finite; a program needn't handle non-finite values.
Results may differ from the reference program's by a relative error of at most 0.02.
Values are sent between devices in bfloat16 or wider.
A program may use at most 768 MiB of HBM per device.

```python
import math
import jax
import jax.numpy as jnp
from jax import lax

BATCH_SIZE = 3
SEQ_LEN = 1536
MODEL_DIM = 2048
NUM_HEADS = 8
HEAD_DIM = 256
FFN_DIM = 16384


def rms_norm(x_in, gain):
    x_f = x_in.astype(jnp.float32)
    inv_rms = lax.rsqrt(jnp.mean(x_f * x_f, axis=-1, keepdims=True) + 1e-6)
    return (x_f * inv_rms * (1.0 + gain.astype(jnp.float32))).astype(jnp.bfloat16)


def rope_tables(positions, head_dim):
    half_dim = head_dim // 2
    exponent = jnp.arange(half_dim, dtype=jnp.float32) * (2.0 / head_dim)
    inv_freq = jnp.exp(exponent * (-math.log(10000.0)))
    angles = positions.astype(jnp.float32)[:, None] * inv_freq[None, :]
    return jnp.cos(angles), jnp.sin(angles)


def apply_rope(x_f, cos_t, sin_t):
    half_dim = x_f.shape[-1] // 2
    first = x_f[..., :half_dim]
    second = x_f[..., half_dim:]
    return jnp.concatenate([first * cos_t - second * sin_t, second * cos_t + first * sin_t], axis=-1)


def attend_one(operands):
    query, keys, values, prefix_count, valid_count = operands
    seq_len = query.shape[0]
    scale = query.shape[-1] ** -0.5
    scores = jnp.einsum("qhd,kd->hqk", query.astype(jnp.float32), keys.astype(jnp.float32)) * scale
    q_pos = jnp.arange(seq_len)[:, None]
    k_pos = jnp.arange(seq_len)[None, :]
    visible = (k_pos < valid_count) & ((k_pos < prefix_count) | (k_pos <= q_pos))
    scores = jnp.where(visible[None], scores, -1e30)
    probs = jax.nn.softmax(scores, axis=-1).astype(jnp.bfloat16)
    mixed = jnp.einsum("hqk,kd->qhd", probs.astype(jnp.float32), values.astype(jnp.float32))
    return mixed.astype(jnp.bfloat16)


def layer_forward(hidden, prefix_len, valid_len, weights):
    attn_norm, w_query, w_key, w_value, w_out, mlp_norm, w_gate, w_up, w_down = weights
    batch, seq_len, model_dim = hidden.shape
    head_dim = w_key.shape[1]
    num_heads = w_query.shape[1] // head_dim
    num_rows = batch * seq_len
    normed = rms_norm(hidden, attn_norm).reshape(num_rows, model_dim)
    cos_t, sin_t = rope_tables(jnp.arange(seq_len), head_dim)
    q_raw = jnp.dot(normed, w_query, preferred_element_type=jnp.float32).reshape(batch, seq_len, num_heads, head_dim)
    query = apply_rope(q_raw, cos_t[:, None, :], sin_t[:, None, :]).astype(jnp.bfloat16)
    k_raw = jnp.dot(normed, w_key, preferred_element_type=jnp.float32).reshape(batch, seq_len, head_dim)
    keys = apply_rope(k_raw, cos_t, sin_t).astype(jnp.bfloat16)
    values = jnp.dot(normed, w_value, preferred_element_type=jnp.float32).astype(jnp.bfloat16).reshape(batch, seq_len, head_dim)
    mixed = lax.map(jax.checkpoint(attend_one), (query, keys, values, prefix_len, valid_len))
    attn_out = jnp.dot(mixed.reshape(num_rows, num_heads * head_dim), w_out, preferred_element_type=jnp.float32)
    resid = (hidden.astype(jnp.float32) + attn_out.reshape(batch, seq_len, model_dim)).astype(jnp.bfloat16)
    gated_in = rms_norm(resid, mlp_norm).reshape(num_rows, model_dim)
    gate = jnp.dot(gated_in, w_gate, preferred_element_type=jnp.float32)
    upper = jnp.dot(gated_in, w_up, preferred_element_type=jnp.float32)
    act = (jax.nn.gelu(gate, approximate=True) * upper).astype(jnp.bfloat16)
    mlp_out = jnp.dot(act, w_down, preferred_element_type=jnp.float32)
    return (resid.astype(jnp.float32) + mlp_out.reshape(batch, seq_len, model_dim)).astype(jnp.bfloat16)


def setup_inputs(seed: int = 0, part: int = 0) -> dict:
    base_key = jax.random.key(seed)
    part_keys = jax.random.split(jax.random.fold_in(base_key, part), 4)
    shared_keys = jax.random.split(base_key, 9)
    q_dim = NUM_HEADS * HEAD_DIM
    act_shape = (BATCH_SIZE, SEQ_LEN, MODEL_DIM)
    hidden = (0.25 * jax.random.normal(part_keys[0], act_shape, jnp.float32)).astype(jnp.bfloat16)
    grad_out = jax.random.normal(part_keys[1], act_shape, jnp.float32).astype(jnp.bfloat16)
    valid_len = jax.random.randint(part_keys[2], (BATCH_SIZE,), (3 * SEQ_LEN) // 4, SEQ_LEN + 1, dtype=jnp.int32)
    valid_len = valid_len.at[0].set(SEQ_LEN)
    prefix_len = jax.random.randint(part_keys[3], (BATCH_SIZE,), SEQ_LEN // 8, (3 * SEQ_LEN) // 4 + 1, dtype=jnp.int32)
    in_scale = 1.0 / math.sqrt(MODEL_DIM)
    out_scale = math.sqrt(SEQ_LEN / (64.0 * q_dim))
    down_scale = 1.0 / math.sqrt(FFN_DIM)
    attn_norm = (0.3 * jax.random.normal(shared_keys[0], (MODEL_DIM,), jnp.float32)).astype(jnp.bfloat16)
    w_query = (in_scale * jax.random.normal(shared_keys[1], (MODEL_DIM, q_dim), jnp.float32)).astype(jnp.bfloat16)
    w_key = (in_scale * jax.random.normal(shared_keys[2], (MODEL_DIM, HEAD_DIM), jnp.float32)).astype(jnp.bfloat16)
    w_value = (in_scale * jax.random.normal(shared_keys[3], (MODEL_DIM, HEAD_DIM), jnp.float32)).astype(jnp.bfloat16)
    w_out = (out_scale * jax.random.normal(shared_keys[4], (q_dim, MODEL_DIM), jnp.float32)).astype(jnp.bfloat16)
    mlp_norm = (0.3 * jax.random.normal(shared_keys[5], (MODEL_DIM,), jnp.float32)).astype(jnp.bfloat16)
    w_gate = (in_scale * jax.random.normal(shared_keys[6], (MODEL_DIM, FFN_DIM), jnp.float32)).astype(jnp.bfloat16)
    w_up = (in_scale * jax.random.normal(shared_keys[7], (MODEL_DIM, FFN_DIM), jnp.float32)).astype(jnp.bfloat16)
    w_down = (down_scale * jax.random.normal(shared_keys[8], (FFN_DIM, MODEL_DIM), jnp.float32)).astype(jnp.bfloat16)
    return {"hidden": hidden, "grad_out": grad_out, "prefix_len": prefix_len, "valid_len": valid_len, "attn_norm": attn_norm, "w_query": w_query, "w_key": w_key, "w_value": w_value, "w_out": w_out, "mlp_norm": mlp_norm, "w_gate": w_gate, "w_up": w_up, "w_down": w_down}


def reference(hidden, grad_out, prefix_len, valid_len, attn_norm, w_query, w_key, w_value, w_out, mlp_norm, w_gate, w_up, w_down):
    weights = (attn_norm, w_query, w_key, w_value, w_out, mlp_norm, w_gate, w_up, w_down)

    def forward(hidden_in, weights_in):
        return layer_forward(hidden_in, prefix_len, valid_len, weights_in)

    hidden_out, pullback = jax.vjp(forward, hidden, weights)
    grad_hidden, grad_weights = pullback(grad_out)
    g_attn_norm, g_query, g_key, g_value, g_out, g_mlp_norm, g_gate, g_up, g_down = grad_weights
    return (hidden_out, grad_hidden, g_attn_norm.astype(jnp.float32), g_query.astype(jnp.float32), g_key.astype(jnp.float32), g_value.astype(jnp.float32), g_out.astype(jnp.float32), g_mlp_norm.astype(jnp.float32), g_gate.astype(jnp.float32), g_up.astype(jnp.float32), g_down.astype(jnp.float32))
```

```python
import math
import jax
import jax.numpy as jnp
from jax import lax
from jax.experimental import pallas as pl
from jax.experimental.pallas import tpu as pltpu
from jax.sharding import PartitionSpec as P

NORM_EPS = 1e-6
F32 = jnp.float32
BF16 = jnp.bfloat16
VMEM_LIMIT = 60 * 1024 * 1024
NN = (((1,), (0,)), ((), ()))
NT = (((1,), (1,)), ((), ()))
TN = (((0,), (0,)), ((), ()))


def dot(a, b, dims=NN):
    return lax.dot_general(a, b, dims, preferred_element_type=F32)


def rms_norm(x_in, gain):
    x_f = x_in.astype(F32)
    inv_rms = lax.rsqrt(jnp.mean(x_f * x_f, axis=-1, keepdims=True) + NORM_EPS)
    return (x_f * inv_rms * (1.0 + gain)).astype(BF16)


def rope_tables(positions, head_dim):
    half_dim = head_dim // 2
    exponent = jnp.arange(half_dim, dtype=F32) * (2.0 / head_dim)
    inv_freq = jnp.exp(exponent * (-math.log(10000.0)))
    angles = positions.astype(F32)[:, None] * inv_freq[None, :]
    return jnp.cos(angles), jnp.sin(angles)


def rotate(x_f, cos_t, sin_t):
    half_dim = x_f.shape[-1] // 2
    first = x_f[..., :half_dim]
    second = x_f[..., half_dim:]
    return jnp.concatenate([first * cos_t - second * sin_t, second * cos_t + first * sin_t], axis=-1)


def params(*semantics):
    return pltpu.CompilerParams(dimension_semantics=semantics, vmem_limit_bytes=VMEM_LIMIT)


def cost(flops, nbytes):
    return pl.CostEstimate(flops=int(flops), bytes_accessed=int(nbytes), transcendentals=0)


def rows_to_heads(x_in, weights, plane, group, tables=None):
    batch, rows, depth = x_in.shape
    heads, _, width, _ = weights.shape

    def kernel(x_ref, w_ref, *refs):
        o_ref = refs[-1]
        x_all = x_ref[...].reshape(batch * rows, depth)
        raw = dot(x_all, w_ref[...].reshape(group * width, depth), NT)
        for n in range(group):
            one = raw[:, n * width:(n + 1) * width].reshape(batch, rows, width)
            if tables is not None:
                one = rotate(one, refs[0][...], refs[1][...])
            o_ref[:, n] = one.astype(BF16)

    table_spec = pl.BlockSpec((rows, width // 2), lambda n: (0, 0))
    return pl.pallas_call(
        kernel,
        out_shape=jax.ShapeDtypeStruct((batch, heads, rows, width), BF16),
        grid=(heads // group,),
        in_specs=[
            pl.BlockSpec((batch, rows, depth), lambda n: (0, 0, 0)),
            pl.BlockSpec((group, 1, width, depth), lambda n: (n, plane, 0, 0)),
        ] + [table_spec] * (0 if tables is None else 2),
        out_specs=pl.BlockSpec((batch, group, rows, width), lambda n: (0, n, 0, 0)),
        compiler_params=params("arbitrary"),
        cost_estimate=cost(2 * batch * rows * depth * heads * width, 2 * heads * depth * width),
        name="rows_to_heads",
    )(x_in, weights, *(() if tables is None else tables))


def heads_to_rows(x_heads, weights, tile):
    batch, heads, rows, width = x_heads.shape
    depth = weights.shape[3]

    def kernel(x_ref, w_ref, o_ref):
        total = None
        for n in range(heads):
            term = dot(x_ref[:, n].reshape(batch * rows, width), w_ref[n, 0])
            total = term if total is None else total + term
        o_ref[...] = total.reshape(batch, rows, tile)

    return pl.pallas_call(
        kernel,
        out_shape=jax.ShapeDtypeStruct((batch, rows, depth), F32),
        grid=(depth // tile,),
        in_specs=[
            pl.BlockSpec((batch, heads, rows, width), lambda j: (0, 0, 0, 0)),
            pl.BlockSpec((heads, 1, width, tile), lambda j: (0, 1, 0, j)),
        ],
        out_specs=pl.BlockSpec((batch, rows, tile), lambda j: (0, 0, j)),
        compiler_params=params("arbitrary"),
        cost_estimate=cost(2 * batch * rows * depth * heads * width, 2 * heads * depth * width),
        name="heads_to_rows",
    )(x_heads, weights)


def input_grad(dq_heads, d_kv, weights, w_key, w_value, tile):
    batch, heads, rows, width = dq_heads.shape
    depth = weights.shape[3]

    def kernel(q_ref, kv_ref, w_ref, wk_ref, wv_ref, o_ref):
        kv_all = kv_ref[...].reshape(batch * rows, 2 * width)
        total = dot(kv_all[:, :width], wk_ref[...], NT) + dot(kv_all[:, width:], wv_ref[...], NT)
        for n in range(heads):
            total = total + dot(q_ref[:, n].reshape(batch * rows, width), w_ref[n, 0])
        o_ref[...] = total.reshape(batch, rows, tile).astype(BF16)

    return pl.pallas_call(
        kernel,
        out_shape=jax.ShapeDtypeStruct((batch, rows, depth), BF16),
        grid=(depth // tile,),
        in_specs=[
            pl.BlockSpec((batch, heads, rows, width), lambda j: (0, 0, 0, 0)),
            pl.BlockSpec((batch, rows, 2 * width), lambda j: (0, 0, 0)),
            pl.BlockSpec((heads, 1, width, tile), lambda j: (0, 0, 0, j)),
            pl.BlockSpec((tile, width), lambda j: (j, 0)),
            pl.BlockSpec((tile, width), lambda j: (j, 0)),
        ],
        out_specs=pl.BlockSpec((batch, rows, tile), lambda j: (0, 0, j)),
        compiler_params=params("arbitrary"),
        cost_estimate=cost(2 * batch * rows * depth * (heads + 2) * width, 2 * heads * depth * width),
        name="input_grad",
    )(dq_heads, d_kv, weights, w_key, w_value)


def out_weight_grad(mixed, d_rows):
    batch, heads, rows, width = mixed.shape
    depth = d_rows.shape[2]

    def kernel(a_ref, d_ref, o_ref):
        left = a_ref[:, 0].reshape(batch * rows, width).T
        o_ref[0] = dot(left, d_ref[...].reshape(batch * rows, depth))

    return pl.pallas_call(
        kernel,
        out_shape=jax.ShapeDtypeStruct((heads, width, depth), F32),
        grid=(heads,),
        in_specs=[
            pl.BlockSpec((batch, 1, rows, width), lambda n: (0, n, 0, 0)),
            pl.BlockSpec((batch, rows, depth), lambda n: (0, 0, 0)),
        ],
        out_specs=pl.BlockSpec((1, width, depth), lambda n: (n, 0, 0)),
        compiler_params=params("arbitrary"),
        cost_estimate=cost(2 * batch * rows * depth * heads * width, 4 * heads * depth * width),
        name="out_weight_grad",
    )(mixed, d_rows)


def query_weight_grad(normed, dq_heads):
    batch, heads, rows, width = dq_heads.shape
    depth = normed.shape[2]

    def kernel(u_ref, dq_ref, o_ref, ut_ref):
        @pl.when(pl.program_id(0) == 0)
        def _():
            ut_ref[...] = u_ref[...].reshape(batch * rows, depth).T

        o_ref[0] = dot(ut_ref[...], dq_ref[:, 0].reshape(batch * rows, width))

    return pl.pallas_call(
        kernel,
        out_shape=jax.ShapeDtypeStruct((heads, depth, width), F32),
        grid=(heads,),
        in_specs=[
            pl.BlockSpec((batch, rows, depth), lambda n: (0, 0, 0)),
            pl.BlockSpec((batch, 1, rows, width), lambda n: (0, n, 0, 0)),
        ],
        out_specs=pl.BlockSpec((1, depth, width), lambda n: (n, 0, 0)),
        scratch_shapes=[pltpu.VMEM((depth, batch * rows), BF16)],
        compiler_params=params("arbitrary"),
        cost_estimate=cost(2 * batch * rows * depth * heads * width, 4 * heads * depth * width),
        name="query_weight_grad",
    )(normed, dq_heads)


def fill_bias(lens_ref, bias_ref, rows, c):
    first, prefix, valid = lens_ref[0], lens_ref[1 + 2 * c], lens_ref[2 + 2 * c]
    key_pos = lax.broadcasted_iota(jnp.int32, bias_ref.shape, 0)
    column = lax.broadcasted_iota(jnp.int32, bias_ref.shape, 1)
    q_pos = first + lax.rem(column, rows)
    visible = (key_pos < valid) & ((key_pos < prefix) | (key_pos <= q_pos))
    bias_ref[...] = jnp.where(visible, 0.0, -1e30).astype(F32)


def attention_fwd(q_heads, keys_values, lens, group, block):
    batch, heads, rows, width = q_heads.shape
    length = keys_values.shape[1]
    cols = group * rows
    scale = width ** -0.5

    def kernel(lens_ref, q_ref, k_ref, v_ref, o_ref, lse_ref, bias_ref, vt_ref, score_ref):
        c, g = pl.program_id(0), pl.program_id(1)

        @pl.when(g == 0)
        def _():
            fill_bias(lens_ref, bias_ref, rows, c)
            vt_ref[...] = v_ref[0].T

        q_s = q_ref[0].reshape(cols, width) * jnp.asarray(scale, BF16)
        top = jnp.full((1, cols), -jnp.inf, F32)
        for at in range(0, length, block):
            scores = dot(k_ref[0, at:at + block], q_s, NT) + bias_ref[at:at + block]
            score_ref[at:at + block] = scores
            top = jnp.maximum(top, jnp.max(scores, axis=0, keepdims=True))
        total = jnp.zeros((1, cols), F32)
        for at in range(0, length, block):
            probs = jnp.exp(score_ref[at:at + block] - top)
            score_ref[at:at + block] = probs
            total = total + jnp.sum(probs, axis=0, keepdims=True)
        lse_ref[0] = top + jnp.log(total)
        inverse = 1.0 / total
        out = None
        for at in range(0, length, block):
            term = dot(vt_ref[:, at:at + block], (score_ref[at:at + block] * inverse).astype(BF16))
            out = term if out is None else out + term
        o_ref[0] = out.T.astype(BF16).reshape(group, rows, width)

    return pl.pallas_call(
        kernel,
        out_shape=(
            jax.ShapeDtypeStruct((batch, heads, rows, width), BF16),
            jax.ShapeDtypeStruct((batch, 1, heads * rows), F32),
        ),
        grid_spec=pltpu.PrefetchScalarGridSpec(
            num_scalar_prefetch=1,
            grid=(batch, heads // group),
            in_specs=[
                pl.BlockSpec((1, group, rows, width), lambda c, g, s: (c, g, 0, 0)),
                pl.BlockSpec((1, length, width), lambda c, g, s: (c, 0, 0)),
                pl.BlockSpec((1, length, width), lambda c, g, s: (c, 0, 1)),
            ],
            out_specs=(
                pl.BlockSpec((1, group, rows, width), lambda c, g, s: (c, g, 0, 0)),
                pl.BlockSpec((1, 1, cols), lambda c, g, s: (c, 0, g)),
            ),
            scratch_shapes=[pltpu.VMEM((length, cols), F32), pltpu.VMEM((width, length), BF16), pltpu.VMEM((length, cols), F32)],
        ),
        compiler_params=params("arbitrary", "arbitrary"),
        cost_estimate=cost(4 * batch * heads * rows * length * width, 16 * batch * heads * rows * width),
        name="attention_fwd",
    )(lens, q_heads, keys_values, keys_values)


def attention_bwd(q_heads, keys_values, mixed, d_mixed, lse, cos_t, sin_t, lens, group, block, start):
    _, heads, rows, width = q_heads.shape
    batch = d_mixed.shape[0]
    length = keys_values.shape[1]
    cols = group * rows
    groups = heads // group
    scale = width ** -0.5

    def kernel(lens_ref, q_ref, k_ref, v_ref, mixed_ref, dm_ref, lse_ref, cos_ref, sin_ref, dq_ref, dkv_ref, bias_ref, kt_ref, acc_ref):
        c, g = pl.program_id(0), pl.program_id(1)

        @pl.when(g == 0)
        def _():
            fill_bias(lens_ref, bias_ref, rows, c + start)
            kt_ref[...] = k_ref[0].T
            acc_ref[...] = jnp.zeros_like(acc_ref)

        q_s = q_ref[0].reshape(cols, width) * jnp.asarray(scale, BF16)
        d_m = dm_ref[0].reshape(cols, width)
        inner = d_m.astype(F32) * mixed_ref[0].reshape(cols, width).astype(F32)
        inner = jnp.sum(inner.T, axis=0, keepdims=True)
        d_q = None
        for at in range(0, length, block):
            here = slice(at, at + block)
            probs = jnp.exp(dot(k_ref[0, here], q_s, NT) + bias_ref[here] - lse_ref[0])
            d_scores = (probs * (dot(v_ref[0, here], d_m, NT) - inner)).astype(BF16)
            acc_ref[here, :width] += dot(d_scores, q_s)
            acc_ref[here, width:] += dot(probs.astype(BF16), d_m)
            term = dot(kt_ref[:, here], d_scores)
            d_q = term if d_q is None else d_q + term
        d_q = (d_q * scale).T.reshape(group, rows, width)
        dq_ref[0] = rotate(d_q, cos_ref[...], -sin_ref[...]).astype(BF16)

        @pl.when(g == groups - 1)
        def _():
            dkv_ref[0] = acc_ref[...].astype(BF16)

    return pl.pallas_call(
        kernel,
        out_shape=(
            jax.ShapeDtypeStruct((batch, heads, rows, width), BF16),
            jax.ShapeDtypeStruct((batch, length, 2 * width), BF16),
        ),
        grid_spec=pltpu.PrefetchScalarGridSpec(
            num_scalar_prefetch=1,
            grid=(batch, groups),
            in_specs=[
                pl.BlockSpec((1, group, rows, width), lambda c, g, s: (c + start, g, 0, 0)),
                pl.BlockSpec((1, length, width), lambda c, g, s: (c + start, 0, 0)),
                pl.BlockSpec((1, length, width), lambda c, g, s: (c + start, 0, 1)),
                pl.BlockSpec((1, group, rows, width), lambda c, g, s: (c + start, g, 0, 0)),
                pl.BlockSpec((1, group, rows, width), lambda c, g, s: (c, g, 0, 0)),
                pl.BlockSpec((1, 1, cols), lambda c, g, s: (c + start, 0, g)),
                pl.BlockSpec((rows, width // 2), lambda c, g, s: (0, 0)),
                pl.BlockSpec((rows, width // 2), lambda c, g, s: (0, 0)),
            ],
            out_specs=(
                pl.BlockSpec((1, group, rows, width), lambda c, g, s: (c, g, 0, 0)),
                pl.BlockSpec((1, length, 2 * width), lambda c, g, s: (c, 0, 0)),
            ),
            scratch_shapes=[
                pltpu.VMEM((length, cols), F32),
                pltpu.VMEM((width, length), BF16),
                pltpu.VMEM((length, 2 * width), F32),
            ],
        ),
        compiler_params=params("arbitrary", "arbitrary"),
        cost_estimate=cost(10 * batch * heads * rows * length * width, 16 * batch * heads * rows * width),
        name="attention_bwd",
    )(lens, q_heads, keys_values, keys_values, mixed, d_mixed, lse, cos_t, sin_t)


def gelu_and_slope(gate):
    root = math.sqrt(2.0 / math.pi)
    square = gate * gate
    tanh = jnp.tanh(root * gate * (1.0 + 0.044715 * square))
    half = 0.5 * (1.0 + tanh)
    slope = half + 0.5 * gate * (1.0 - tanh * tanh) * (root * (1.0 + 3 * 0.044715 * square))
    return gate * half, slope


def mlp_core(z_seq, g_seq, w_gate, w_up, w_down, tm, tn):
    _, rows, depth = z_seq[0].shape
    width = w_gate.shape[1]

    def kernel(z_ref, g_ref, wg_ref, wu_ref, wd_ref, act_ref, dg_ref, du_ref):
        gate = dot(z_ref[0], wg_ref[...])
        upper = dot(z_ref[0], wu_ref[...])
        d_act = dot(g_ref[0], wd_ref[...], NT).astype(BF16).astype(F32)
        gelu, slope = gelu_and_slope(gate)
        act_ref[...] = (gelu * upper).astype(BF16)
        dg_ref[...] = (d_act * upper * slope).astype(BF16)
        du_ref[...] = (d_act * gelu).astype(BF16)

    def row_spec(k):
        return pl.BlockSpec((1, tm, depth), lambda i, j: (k, i, 0))

    col_spec = pl.BlockSpec((depth, tn), lambda i, j: (0, j))
    out_spec = pl.BlockSpec((tm, tn), lambda i, j: (i, j))
    out = jax.ShapeDtypeStruct((rows, width), BF16)
    return pl.pallas_call(
        kernel,
        out_shape=(out, out, out),
        grid=(rows // tm, width // tn),
        in_specs=[row_spec(z_seq[1]), row_spec(g_seq[1]), col_spec, col_spec, pl.BlockSpec((tn, depth), lambda i, j: (j, 0))],
        out_specs=(out_spec, out_spec, out_spec),
        compiler_params=params("arbitrary", "arbitrary"),
        cost_estimate=cost(6 * rows * depth * width, 6 * depth * width + 10 * rows * depth),
        name="mlp_core",
    )(z_seq[0], g_seq[0], w_gate, w_up, w_down)


def product_sum(lefts, rights, dims, out_dtype, tm, tn):
    rows, depth = lefts[0].shape
    width = rights[0].shape[0] if dims == NT else rights[0].shape[1]
    count = len(lefts)

    def kernel(*refs):
        total = dot(refs[0][...], refs[count][...], dims)
        for i in range(1, count):
            total = total + dot(refs[i][...], refs[count + i][...], dims)
        refs[-1][...] = total.astype(out_dtype)

    left_spec = pl.BlockSpec((tm, depth), lambda i, j: (i, 0))
    if dims == NT:
        right_spec = pl.BlockSpec((tn, depth), lambda i, j: (j, 0))
    else:
        right_spec = pl.BlockSpec((depth, tn), lambda i, j: (0, j))
    return pl.pallas_call(
        kernel,
        out_shape=jax.ShapeDtypeStruct((rows, width), out_dtype),
        grid=(rows // tm, width // tn),
        in_specs=[left_spec] * count + [right_spec] * count,
        out_specs=pl.BlockSpec((tm, tn), lambda i, j: (i, j)),
        compiler_params=params("arbitrary", "arbitrary"),
        cost_estimate=cost(2 * count * rows * depth * width, 2 * count * depth * (rows + width)),
    )(*lefts, *rights)


def split_product(lefts, right, core, chips, tm, tn):
    rows, depth = lefts[0].shape
    width = right.shape[1]
    count, steps = len(lefts), rows // tm
    shard = rows // (2 * chips)
    here = tm // (2 * shard)

    def kernel(core_ref, *refs):
        c = pl.program_id(0)
        for k in range(count):
            @pl.when(c == k)
            def _(k=k):
                product = dot(refs[k][...], refs[count][...]).astype(BF16).reshape(here, 2, shard, tn)
                first = core_ref[0] == 0
                refs[-2][:, 0] = jnp.where(first, product[:, 0], product[:, 1])
                refs[-1][:, 0] = jnp.where(first, product[:, 1], product[:, 0])

    def left_spec(k):
        return pl.BlockSpec((tm, depth), lambda c, i, j, s: (jnp.where(c == k, i, jnp.where(c < k, 0, steps - 1)), 0))

    out = jax.ShapeDtypeStruct((chips, count, shard, width), BF16)
    out_spec = pl.BlockSpec((here, 1, shard, tn), lambda c, i, j, s: (i, c, 0, j))
    return pl.pallas_call(
        kernel,
        out_shape=(out, out),
        grid_spec=pltpu.PrefetchScalarGridSpec(
            num_scalar_prefetch=1,
            grid=(count, steps, width // tn),
            in_specs=[left_spec(k) for k in range(count)] + [pl.BlockSpec((depth, tn), lambda c, i, j, s: (0, j))],
            out_specs=(out_spec, out_spec),
        ),
        compiler_params=params("arbitrary", "arbitrary", "arbitrary"),
        cost_estimate=cost(2 * count * rows * depth * width, 2 * count * rows * (depth + width)),
        name="mlp_out",
    )(core[None], *lefts, right)


def weight_grad(lefts, rights, tm, tn):
    _, rows, depth = lefts[0][0].shape
    width = rights[0][0].shape[2]
    count = len(lefts)

    def kernel(*refs):
        total = None
        for c in range(count):
            term = dot(refs[c][0], refs[count + c][0], TN)
            total = term if total is None else total + term
        refs[-1][...] = total

    def left_spec(k):
        return pl.BlockSpec((1, rows, tm), lambda i, j: (k, 0, i))

    def right_spec(k):
        return pl.BlockSpec((1, rows, tn), lambda i, j: (k, 0, j))

    return pl.pallas_call(
        kernel,
        out_shape=jax.ShapeDtypeStruct((depth, width), F32),
        grid=(depth // tm, width // tn),
        in_specs=[left_spec(k) for _, k in lefts] + [right_spec(k) for _, k in rights],
        out_specs=pl.BlockSpec((tm, tn), lambda i, j: (i, j)),
        compiler_params=params("arbitrary", "arbitrary"),
        cost_estimate=cost(2 * count * rows * depth * width, 2 * count * rows * (depth + width)),
        name="weight_grad",
    )(*[a for a, _ in lefts], *[a for a, _ in rights])


def chip_shift(x_in, step, size):
    return lax.ppermute(x_in, "tp", [(t, (t + 2 * step) % size) for t in range(size)])


def swap_cores(x_in, size):
    return lax.ppermute(x_in, "tp", [(t, t ^ 1) for t in range(size)])


def scatter_by_sends(keep, arrived, chip, size, marks):
    chips, count, shard, depth = keep.shape
    half = shard // 2
    arrived = after(arrived, marks[0])

    def pair_sum(step):
        at = ((chip + step) % chips, 0, 0, 0)
        cut = (1, count, shard, depth)
        return lax.dynamic_slice(keep, at, cut)[0].astype(F32) + lax.dynamic_slice(arrived, at, cut)[0].astype(F32)

    far = pair_sum(2).astype(BF16)
    far_low = after(chip_shift(far[:, :half], 1, size), marks[1])
    far_high = after(chip_shift(far[:, half:], -1, size), marks[1])
    forward, backward = pair_sum(1), pair_sum(-1)
    forward = jnp.concatenate([forward[:, :half] + far_low.astype(F32), forward[:, half:]], axis=1).astype(BF16)
    backward = jnp.concatenate([backward[:, :half], backward[:, half:] + far_high.astype(F32)], axis=1).astype(BF16)
    forward = after(chip_shift(forward, 1, size), marks[2])
    backward = after(chip_shift(backward, -1, size), marks[2])
    return pair_sum(0) + forward.astype(F32) + backward.astype(F32)


def gather(x_loc, axis):
    return lax.all_gather(x_loc, "tp", axis=axis, tiled=True)


def after(value, earlier):
    return lax.optimization_barrier((value, earlier))[0]


def scatter(x_part, axis):
    return lax.psum_scatter(x_part, "tp", scatter_dimension=axis, tiled=True)


def solution(mesh):
    tp_size = mesh.shape["tp"]
    act_spec = P("dp", "tp", None)
    in_specs = (act_spec, act_spec, P("dp"), P("dp"), P(None), P(None, "tp"), P(None, None), P(None, None), P("tp", None), P(None), P(None, "tp"), P(None, "tp"), P("tp", None))
    out_specs = (act_spec, act_spec, P("dp"), P("dp", "tp"), P("dp", None), P("dp", None), P(("dp", "tp"), None), P("dp"), P("dp", "tp"), P("dp", "tp"), P(("dp", "tp"), None))

    def local_layer(hidden, grad_out, prefix_len, valid_len, attn_norm, w_query, w_key, w_value, w_out, mlp_norm, w_gate, w_up, w_down):
        batch, shard_len, model_dim = hidden.shape
        head_dim = w_key.shape[1]
        heads = tp_size * w_query.shape[1] // head_dim
        first = lax.axis_index("tp") * shard_len
        cos_t, sin_t = rope_tables(first + jnp.arange(shard_len), head_dim)
        lens = jnp.concatenate([first[None].astype(jnp.int32), jnp.stack([prefix_len, valid_len], axis=1).reshape(-1).astype(jnp.int32)])

        weights = gather(jnp.stack([w_query.T, w_out])[None], 0)
        normed, norm1_pull = jax.vjp(rms_norm, hidden, attn_norm.astype(F32))
        k_raw = jnp.einsum("bsd,de->bse", normed, w_key, preferred_element_type=F32)
        keys = rotate(k_raw, cos_t, sin_t).astype(BF16)
        values = jnp.einsum("bsd,de->bse", normed, w_value, preferred_element_type=F32).astype(BF16)
        keys_values = gather(jnp.concatenate([keys, values], axis=-1), 1)
        query = rows_to_heads(normed, weights, 0, 2, (cos_t, sin_t))
        mixed, lse = attention_fwd(query, keys_values, lens, 4, 512)
        attn_out = heads_to_rows(mixed, weights, 1024)
        resid = (hidden.astype(F32) + attn_out).astype(BF16)
        gated_in = rms_norm(resid, mlp_norm.astype(F32))

        me = lax.axis_index("tp")
        chip, core = me // 2, me % 2
        z_all, g_all, acts, d_gates, d_ups, d_gated = [], [], [], [], [], []
        for c in range(batch):
            g_c = (gather(grad_out[c:c + 1], 1), 0)
            z_c = (gather(gated_in[c:c + 1], 1), 0)
            if c:
                z_c = (after(z_c[0], d_z_part), 0)
            act, d_gate, d_up = mlp_core(z_c, g_c, w_gate, w_up, w_down, 768, 512)
            d_z_part = product_sum([d_gate, d_up], [w_gate, w_up], NT, BF16, 768, 1024)
            d_gated.append(scatter(d_z_part, 0))
            for items, item in zip((z_all, g_all, acts, d_gates, d_ups), (z_c, g_c, act, d_gate, d_up)):
                items.append(item)

        def planes(arrays):
            return [(a[None], 0) for a in arrays]

        d_resids, norm_parts, dq_parts, d_kv_sums = [], [], [], []
        previous = d_z_part
        for start, stop in ((0, batch - 1), (batch - 1, batch)):
            _, norm2_pull = jax.vjp(rms_norm, resid[start:stop], mlp_norm.astype(F32))
            d_resid_norm, norm_part = norm2_pull(after(jnp.stack(d_gated[start:stop]), previous))
            d_resid = (grad_out[start:stop].astype(F32) + d_resid_norm.astype(F32)).astype(BF16)
            d_mixed = rows_to_heads(d_resid, weights, 1, 2)
            dq_part, d_kv_part = attention_bwd(query, keys_values, mixed, d_mixed, lse, cos_t, sin_t, lens, 4, 512, start)
            d_kv_sums.append(scatter(d_kv_part, 1))
            previous = d_kv_part
            d_resids.append(d_resid)
            norm_parts.append(norm_part)
            dq_parts.append(dq_part)
        d_resid = jnp.concatenate(d_resids, axis=0)
        g_mlp_norm_part = norm_parts[0] + norm_parts[1]
        dq_raw = jnp.concatenate(dq_parts, axis=0)
        d_kv = jnp.concatenate(d_kv_sums, axis=0)

        g_query_part = query_weight_grad(after(normed, d_kv_part), dq_raw)
        g_query = scatter(g_query_part, 0)[0]
        keep, send = split_product(after(acts, g_query_part), w_down, core, tp_size // 2, 768, 1024)
        arrived = swap_cores(send, tp_size)
        d_kv = after(d_kv, keep)
        d_k_raw = rotate(d_kv[..., :head_dim].astype(F32), cos_t, -sin_t).astype(BF16)
        d_kv_raw = jnp.concatenate([d_k_raw, d_kv[..., head_dim:]], axis=-1)
        d_normed = input_grad(dq_raw, d_kv_raw, weights, w_key, w_value, 1024)
        d_hidden_norm, g_attn_norm_part = norm1_pull(d_normed)
        grad_hidden = (d_resid.astype(F32) + d_hidden_norm.astype(F32)).astype(BF16)

        g_kv_part = jnp.einsum("bsd,bse->de", normed, d_kv_raw, preferred_element_type=F32)
        norms = jnp.concatenate([g_attn_norm_part, g_mlp_norm_part]).reshape(-1, 2 * head_dim)
        count = norms.shape[0]
        fill = jnp.zeros((-(model_dim + count) % (8 * heads), 2 * head_dim), F32)
        small_part = jnp.concatenate([g_kv_part, norms, fill], axis=0)
        small = scatter(small_part, 0)
        g_out_part = out_weight_grad(after(mixed, small_part), d_resid)
        g_out = scatter(g_out_part, 0)

        g_down = weight_grad(planes(after(acts, g_out_part)), g_all, 1024, 512)
        g_gate = weight_grad(z_all, planes(after(d_gates, g_down)), 1024, 512)
        g_up = weight_grad(z_all, planes(after(d_ups, g_gate)), 1024, 512)
        mlp_sum = scatter_by_sends(keep, arrived, chip, tp_size, (small_part, g_down, g_up)).astype(BF16)
        hidden_out = (resid.astype(F32) + mlp_sum.astype(F32)).astype(BF16)
        small = gather(after(small, g_gate), 0)
        g_key, g_value = small[:model_dim, :head_dim], small[:model_dim, head_dim:]
        g_norms = small[model_dim:model_dim + count].reshape(2, model_dim)

        return (hidden_out, grad_hidden, g_norms[0], g_query, g_key, g_value, g_out.reshape(-1, model_dim), g_norms[1], g_gate, g_up, g_down)

    return jax.shard_map(local_layer, mesh=mesh, in_specs=in_specs, out_specs=out_specs, check_vma=False)
```

```python
import math
import jax
import jax.numpy as jnp
from jax import lax
from jax.experimental import pallas as pl
from jax.experimental.pallas import tpu as pltpu
from jax.sharding import PartitionSpec as P

NORM_EPS = 1e-6
F32 = jnp.float32
BF16 = jnp.bfloat16
VMEM_LIMIT = 60 * 1024 * 1024
NN = (((1,), (0,)), ((), ()))
NT = (((1,), (1,)), ((), ()))
TN = (((0,), (0,)), ((), ()))


def dot(a, b, dims=NN):
    return lax.dot_general(a, b, dims, preferred_element_type=F32)


def rms_norm(x_in, gain):
    x_f = x_in.astype(F32)
    inv_rms = lax.rsqrt(jnp.mean(x_f * x_f, axis=-1, keepdims=True) + NORM_EPS)
    return (x_f * inv_rms * (1.0 + gain)).astype(BF16)


def rope_tables(positions, head_dim):
    half_dim = head_dim // 2
    exponent = jnp.arange(half_dim, dtype=F32) * (2.0 / head_dim)
    inv_freq = jnp.exp(exponent * (-math.log(10000.0)))
    angles = positions.astype(F32)[:, None] * inv_freq[None, :]
    return jnp.cos(angles), jnp.sin(angles)


def rotate(x_f, cos_t, sin_t):
    half_dim = x_f.shape[-1] // 2
    first = x_f[..., :half_dim]
    second = x_f[..., half_dim:]
    return jnp.concatenate([first * cos_t - second * sin_t, second * cos_t + first * sin_t], axis=-1)


def params(*semantics):
    return pltpu.CompilerParams(dimension_semantics=semantics, vmem_limit_bytes=VMEM_LIMIT)


def cost(flops, nbytes):
    return pl.CostEstimate(flops=int(flops), bytes_accessed=int(nbytes), transcendentals=0)


def slot_specs(slots, width, tile, column):
    return [pl.BlockSpec((1, width, tile), lambda *ids, k=k: (k, 0, column(*ids))) for _, k in slots]


def rows_to_heads(x_in, slots, width, tables=None):
    batch, rows, depth = x_in.shape
    heads = len(slots)

    def kernel(x_ref, *refs):
        o_ref = refs[-1]
        x_all = x_ref[...].reshape(batch * rows, depth)
        for n in range(heads):
            one = dot(x_all, refs[n][0], NT).reshape(batch, rows, width)
            if tables is not None:
                one = rotate(one, refs[heads][...], refs[heads + 1][...])
            o_ref[:, n] = one.astype(BF16)

    table_spec = pl.BlockSpec((rows, width // 2), lambda n: (0, 0))
    return pl.pallas_call(
        kernel,
        out_shape=jax.ShapeDtypeStruct((batch, heads, rows, width), BF16),
        grid=(1,),
        in_specs=[pl.BlockSpec((batch, rows, depth), lambda n: (0, 0, 0))] + slot_specs(slots, width, depth, lambda n: 0)
        + [table_spec] * (0 if tables is None else 2),
        out_specs=pl.BlockSpec((batch, heads, rows, width), lambda n: (0, 0, 0, 0)),
        compiler_params=params("arbitrary"),
        cost_estimate=cost(2 * batch * rows * depth * heads * width, 2 * heads * depth * width),
        name="rows_to_heads",
    )(x_in, *[a for a, _ in slots], *(() if tables is None else tables))


def heads_to_rows(x_heads, slots, depth, tile):
    batch, heads, rows, width = x_heads.shape

    def kernel(x_ref, *refs):
        total = None
        for n in range(heads):
            term = dot(x_ref[:, n].reshape(batch * rows, width), refs[n][0])
            total = term if total is None else total + term
        refs[-1][...] = total.reshape(batch, rows, tile)

    return pl.pallas_call(
        kernel,
        out_shape=jax.ShapeDtypeStruct((batch, rows, depth), F32),
        grid=(depth // tile,),
        in_specs=[pl.BlockSpec((batch, heads, rows, width), lambda j: (0, 0, 0, 0))] + slot_specs(slots, width, tile, lambda j: j),
        out_specs=pl.BlockSpec((batch, rows, tile), lambda j: (0, 0, j)),
        compiler_params=params("arbitrary"),
        cost_estimate=cost(2 * batch * rows * depth * heads * width, 2 * heads * depth * width),
        name="heads_to_rows",
    )(x_heads, *[a for a, _ in slots])


def input_grad(dq_heads, d_kv, slots, w_key, w_value, tile):
    batch, heads, rows, width = dq_heads.shape
    depth = w_key.shape[0]

    def kernel(q_ref, kv_ref, wk_ref, wv_ref, *refs):
        kv_all = kv_ref[...].reshape(batch * rows, 2 * width)
        total = dot(kv_all[:, :width], wk_ref[...], NT) + dot(kv_all[:, width:], wv_ref[...], NT)
        for n in range(heads):
            total = total + dot(q_ref[:, n].reshape(batch * rows, width), refs[n][0])
        refs[-1][...] = total.reshape(batch, rows, tile).astype(BF16)

    return pl.pallas_call(
        kernel,
        out_shape=jax.ShapeDtypeStruct((batch, rows, depth), BF16),
        grid=(depth // tile,),
        in_specs=[
            pl.BlockSpec((batch, heads, rows, width), lambda j: (0, 0, 0, 0)),
            pl.BlockSpec((batch, rows, 2 * width), lambda j: (0, 0, 0)),
            pl.BlockSpec((tile, width), lambda j: (j, 0)),
            pl.BlockSpec((tile, width), lambda j: (j, 0)),
        ] + slot_specs(slots, width, tile, lambda j: j),
        out_specs=pl.BlockSpec((batch, rows, tile), lambda j: (0, 0, j)),
        compiler_params=params("arbitrary"),
        cost_estimate=cost(2 * batch * rows * depth * (heads + 2) * width, 2 * heads * depth * width),
        name="input_grad",
    )(dq_heads, d_kv, w_key, w_value, *[a for a, _ in slots])


def out_weight_grad(mixed, d_rows, ranks):
    batch, heads, rows, width = mixed.shape
    depth = d_rows.shape[2]

    def kernel(rank_ref, a_ref, d_ref, o_ref):
        left = a_ref[:, 0].reshape(batch * rows, width).T
        o_ref[0] = dot(left, d_ref[...].reshape(batch * rows, depth))

    return pl.pallas_call(
        kernel,
        out_shape=jax.ShapeDtypeStruct((heads, width, depth), F32),
        grid_spec=pltpu.PrefetchScalarGridSpec(
            num_scalar_prefetch=1,
            grid=(heads,),
            in_specs=[
                pl.BlockSpec((batch, 1, rows, width), lambda n, s: (0, n, 0, 0)),
                pl.BlockSpec((batch, rows, depth), lambda n, s: (0, 0, 0)),
            ],
            out_specs=pl.BlockSpec((1, width, depth), lambda n, s: (s[n], 0, 0)),
        ),
        compiler_params=params("arbitrary"),
        cost_estimate=cost(2 * batch * rows * depth * heads * width, 4 * heads * depth * width),
        name="out_weight_grad",
    )(ranks, mixed, d_rows)


def query_weight_grad(normed, dq_heads, ranks):
    batch, heads, rows, width = dq_heads.shape
    depth = normed.shape[2]

    def kernel(rank_ref, u_ref, dq_ref, o_ref, ut_ref):
        @pl.when(pl.program_id(0) == 0)
        def _():
            ut_ref[...] = u_ref[...].reshape(batch * rows, depth).T

        o_ref[0] = dot(ut_ref[...], dq_ref[:, 0].reshape(batch * rows, width))

    return pl.pallas_call(
        kernel,
        out_shape=jax.ShapeDtypeStruct((heads, depth, width), F32),
        grid_spec=pltpu.PrefetchScalarGridSpec(
            num_scalar_prefetch=1,
            grid=(heads,),
            in_specs=[
                pl.BlockSpec((batch, rows, depth), lambda n, s: (0, 0, 0)),
                pl.BlockSpec((batch, 1, rows, width), lambda n, s: (0, n, 0, 0)),
            ],
            out_specs=pl.BlockSpec((1, depth, width), lambda n, s: (s[n], 0, 0)),
            scratch_shapes=[pltpu.VMEM((depth, batch * rows), BF16)],
        ),
        compiler_params=params("arbitrary"),
        cost_estimate=cost(2 * batch * rows * depth * heads * width, 4 * heads * depth * width),
        name="query_weight_grad",
    )(ranks, normed, dq_heads)


def small_grads(normed, d_kv, norms):
    batch, rows, depth = normed.shape
    width = d_kv.shape[2]
    extra = norms.shape[0]

    def kernel(u_ref, kv_ref, norm_ref, o_ref):
        o_ref[:depth] = dot(u_ref[...].reshape(batch * rows, depth), kv_ref[...].reshape(batch * rows, width), TN)
        o_ref[depth:] = norm_ref[...]

    return pl.pallas_call(
        kernel,
        out_shape=jax.ShapeDtypeStruct((depth + extra, width), F32),
        compiler_params=pltpu.CompilerParams(vmem_limit_bytes=VMEM_LIMIT),
        cost_estimate=cost(2 * batch * rows * depth * width, 4 * depth * width),
        name="small_grads",
    )(normed, d_kv, norms)


def fill_bias(lens_ref, bias_ref, rows, c):
    first, prefix, valid = lens_ref[0], lens_ref[1 + 2 * c], lens_ref[2 + 2 * c]
    key_pos = lax.broadcasted_iota(jnp.int32, bias_ref.shape, 0)
    column = lax.broadcasted_iota(jnp.int32, bias_ref.shape, 1)
    q_pos = first + lax.rem(column, rows)
    visible = (key_pos < valid) & ((key_pos < prefix) | (key_pos <= q_pos))
    bias_ref[...] = jnp.where(visible, 0.0, -1e30).astype(F32)


def attention_fwd(q_heads, keys_values, lens, group, block, start, batch):
    _, heads, rows, width = q_heads.shape
    length = keys_values.shape[1]
    cols = group * rows
    scale = width ** -0.5

    def kernel(lens_ref, q_ref, k_ref, v_ref, o_ref, lse_ref, bias_ref, vt_ref, score_ref):
        c, g = pl.program_id(0), pl.program_id(1)

        @pl.when(g == 0)
        def _():
            fill_bias(lens_ref, bias_ref, rows, c + start)
            vt_ref[...] = v_ref[0].T

        q_s = q_ref[0].reshape(cols, width) * jnp.asarray(scale, BF16)
        top = jnp.full((1, cols), -jnp.inf, F32)
        for at in range(0, length, block):
            scores = dot(k_ref[0, at:at + block], q_s, NT) + bias_ref[at:at + block]
            score_ref[at:at + block] = scores
            top = jnp.maximum(top, jnp.max(scores, axis=0, keepdims=True))
        total = jnp.zeros((1, cols), F32)
        for at in range(0, length, block):
            probs = jnp.exp(score_ref[at:at + block] - top)
            score_ref[at:at + block] = probs
            total = total + jnp.sum(probs, axis=0, keepdims=True)
        lse_ref[0] = top + jnp.log(total)
        inverse = 1.0 / total
        out = None
        for at in range(0, length, block):
            term = dot(vt_ref[:, at:at + block], (score_ref[at:at + block] * inverse).astype(BF16))
            out = term if out is None else out + term
        o_ref[0] = out.T.astype(BF16).reshape(group, rows, width)

    return pl.pallas_call(
        kernel,
        out_shape=(
            jax.ShapeDtypeStruct((batch, heads, rows, width), BF16),
            jax.ShapeDtypeStruct((batch, 1, heads * rows), F32),
        ),
        grid_spec=pltpu.PrefetchScalarGridSpec(
            num_scalar_prefetch=1,
            grid=(batch, heads // group),
            in_specs=[
                pl.BlockSpec((1, group, rows, width), lambda c, g, s: (c + start, g, 0, 0)),
                pl.BlockSpec((1, length, width), lambda c, g, s: (c + start, 0, 0)),
                pl.BlockSpec((1, length, width), lambda c, g, s: (c + start, 0, 1)),
            ],
            out_specs=(
                pl.BlockSpec((1, group, rows, width), lambda c, g, s: (c, g, 0, 0)),
                pl.BlockSpec((1, 1, cols), lambda c, g, s: (c, 0, g)),
            ),
            scratch_shapes=[pltpu.VMEM((length, cols), F32), pltpu.VMEM((width, length), BF16), pltpu.VMEM((length, cols), F32)],
        ),
        compiler_params=params("arbitrary", "arbitrary"),
        cost_estimate=cost(4 * batch * heads * rows * length * width, 16 * batch * heads * rows * width),
        name="attention_fwd",
    )(lens, q_heads, keys_values, keys_values)


def attention_bwd(q_heads, keys_values, mixed, d_mixed, lse, cos_t, sin_t, lens, group, block, start):
    _, heads, rows, width = q_heads.shape
    batch = d_mixed.shape[0]
    length = keys_values.shape[1]
    cols = group * rows
    groups = heads // group
    scale = width ** -0.5

    def kernel(lens_ref, q_ref, k_ref, v_ref, mixed_ref, dm_ref, lse_ref, cos_ref, sin_ref, dq_ref, dkv_ref, bias_ref, kt_ref, acc_ref):
        c, g = pl.program_id(0), pl.program_id(1)

        @pl.when(g == 0)
        def _():
            fill_bias(lens_ref, bias_ref, rows, c + start)
            kt_ref[...] = k_ref[0].T
            acc_ref[...] = jnp.zeros_like(acc_ref)

        q_s = q_ref[0].reshape(cols, width) * jnp.asarray(scale, BF16)
        d_m = dm_ref[0].reshape(cols, width)
        inner = d_m.astype(F32) * mixed_ref[0].reshape(cols, width).astype(F32)
        inner = jnp.sum(inner.T, axis=0, keepdims=True)
        d_q = None
        for at in range(0, length, block):
            here = slice(at, at + block)
            probs = jnp.exp(dot(k_ref[0, here], q_s, NT) + bias_ref[here] - lse_ref[0])
            d_scores = (probs * (dot(v_ref[0, here], d_m, NT) - inner)).astype(BF16)
            acc_ref[here, :width] += dot(d_scores, q_s)
            acc_ref[here, width:] += dot(probs.astype(BF16), d_m)
            term = dot(kt_ref[:, here], d_scores)
            d_q = term if d_q is None else d_q + term
        d_q = (d_q * scale).T.reshape(group, rows, width)
        dq_ref[0] = rotate(d_q, cos_ref[...], -sin_ref[...]).astype(BF16)

        @pl.when(g == groups - 1)
        def _():
            dkv_ref[0] = acc_ref[...].astype(BF16)

    return pl.pallas_call(
        kernel,
        out_shape=(
            jax.ShapeDtypeStruct((batch, heads, rows, width), BF16),
            jax.ShapeDtypeStruct((batch, length, 2 * width), BF16),
        ),
        grid_spec=pltpu.PrefetchScalarGridSpec(
            num_scalar_prefetch=1,
            grid=(batch, groups),
            in_specs=[
                pl.BlockSpec((1, group, rows, width), lambda c, g, s: (c + start, g, 0, 0)),
                pl.BlockSpec((1, length, width), lambda c, g, s: (c + start, 0, 0)),
                pl.BlockSpec((1, length, width), lambda c, g, s: (c + start, 0, 1)),
                pl.BlockSpec((1, group, rows, width), lambda c, g, s: (c + start, g, 0, 0)),
                pl.BlockSpec((1, group, rows, width), lambda c, g, s: (c, g, 0, 0)),
                pl.BlockSpec((1, 1, cols), lambda c, g, s: (c + start, 0, g)),
                pl.BlockSpec((rows, width // 2), lambda c, g, s: (0, 0)),
                pl.BlockSpec((rows, width // 2), lambda c, g, s: (0, 0)),
            ],
            out_specs=(
                pl.BlockSpec((1, group, rows, width), lambda c, g, s: (c, g, 0, 0)),
                pl.BlockSpec((1, length, 2 * width), lambda c, g, s: (c, 0, 0)),
            ),
            scratch_shapes=[
                pltpu.VMEM((length, cols), F32),
                pltpu.VMEM((width, length), BF16),
                pltpu.VMEM((length, 2 * width), F32),
            ],
        ),
        compiler_params=params("arbitrary", "arbitrary"),
        cost_estimate=cost(10 * batch * heads * rows * length * width, 16 * batch * heads * rows * width),
        name="attention_bwd",
    )(lens, q_heads, keys_values, keys_values, mixed, d_mixed, lse, cos_t, sin_t)


def gelu_and_slope(gate):
    root = math.sqrt(2.0 / math.pi)
    square = gate * gate
    tanh = jnp.tanh(root * gate * (1.0 + 0.044715 * square))
    half = 0.5 * (1.0 + tanh)
    slope = half + 0.5 * gate * (1.0 - tanh * tanh) * (root * (1.0 + 3 * 0.044715 * square))
    return gate * half, slope


def mlp_core(z_seq, g_seq, w_gate, w_up, w_down, tm, tn):
    _, rows, depth = z_seq[0].shape
    width = w_gate.shape[1]

    def kernel(z_ref, g_ref, wg_ref, wu_ref, wd_ref, act_ref, dg_ref, du_ref):
        gate = dot(z_ref[0], wg_ref[...])
        upper = dot(z_ref[0], wu_ref[...])
        d_act = dot(g_ref[0], wd_ref[...], NT).astype(BF16).astype(F32)
        gelu, slope = gelu_and_slope(gate)
        act_ref[...] = (gelu * upper).astype(BF16)
        dg_ref[...] = (d_act * upper * slope).astype(BF16)
        du_ref[...] = (d_act * gelu).astype(BF16)

    def row_spec(k):
        return pl.BlockSpec((1, tm, depth), lambda i, j: (k, i, 0))

    col_spec = pl.BlockSpec((depth, tn), lambda i, j: (0, j))
    out_spec = pl.BlockSpec((tm, tn), lambda i, j: (i, j))
    out = jax.ShapeDtypeStruct((rows, width), BF16)
    return pl.pallas_call(
        kernel,
        out_shape=(out, out, out),
        grid=(rows // tm, width // tn),
        in_specs=[row_spec(z_seq[1]), row_spec(g_seq[1]), col_spec, col_spec, pl.BlockSpec((tn, depth), lambda i, j: (j, 0))],
        out_specs=(out_spec, out_spec, out_spec),
        compiler_params=params("arbitrary", "arbitrary"),
        cost_estimate=cost(6 * rows * depth * width, 6 * depth * width + 10 * rows * depth),
        name="mlp_core",
    )(z_seq[0], g_seq[0], w_gate, w_up, w_down)


def product_sum(lefts, rights, dims, out_dtype, tm, tn):
    rows, depth = lefts[0].shape
    width = rights[0].shape[0] if dims == NT else rights[0].shape[1]
    count = len(lefts)

    def kernel(*refs):
        total = dot(refs[0][...], refs[count][...], dims)
        for i in range(1, count):
            total = total + dot(refs[i][...], refs[count + i][...], dims)
        refs[-1][...] = total.astype(out_dtype)

    left_spec = pl.BlockSpec((tm, depth), lambda i, j: (i, 0))
    if dims == NT:
        right_spec = pl.BlockSpec((tn, depth), lambda i, j: (j, 0))
    else:
        right_spec = pl.BlockSpec((depth, tn), lambda i, j: (0, j))
    return pl.pallas_call(
        kernel,
        out_shape=jax.ShapeDtypeStruct((rows, width), out_dtype),
        grid=(rows // tm, width // tn),
        in_specs=[left_spec] * count + [right_spec] * count,
        out_specs=pl.BlockSpec((tm, tn), lambda i, j: (i, j)),
        compiler_params=params("arbitrary", "arbitrary"),
        cost_estimate=cost(2 * count * rows * depth * width, 2 * count * depth * (rows + width)),
    )(*lefts, *rights)


def split_product(lefts, right, core, chips, tm, tn):
    rows, depth = lefts[0].shape
    width = right.shape[1]
    count, steps = len(lefts), rows // tm
    shard = rows // (2 * chips)
    here = tm // (2 * shard)

    def kernel(core_ref, *refs):
        c = pl.program_id(0)
        for k in range(count):
            @pl.when(c == k)
            def _(k=k):
                product = dot(refs[k][...], refs[count][...]).astype(BF16).reshape(here, 2, shard, tn)
                first = core_ref[0] == 0
                refs[-2][:, 0] = jnp.where(first, product[:, 0], product[:, 1])
                refs[-1][:, 0] = jnp.where(first, product[:, 1], product[:, 0])

    def left_spec(k):
        return pl.BlockSpec((tm, depth), lambda c, i, j, s: (jnp.where(c == k, i, jnp.where(c < k, 0, steps - 1)), 0))

    out = jax.ShapeDtypeStruct((chips, count, shard, width), BF16)
    out_spec = pl.BlockSpec((here, 1, shard, tn), lambda c, i, j, s: (i, c, 0, j))
    return pl.pallas_call(
        kernel,
        out_shape=(out, out),
        grid_spec=pltpu.PrefetchScalarGridSpec(
            num_scalar_prefetch=1,
            grid=(count, steps, width // tn),
            in_specs=[left_spec(k) for k in range(count)] + [pl.BlockSpec((depth, tn), lambda c, i, j, s: (0, j))],
            out_specs=(out_spec, out_spec),
        ),
        compiler_params=params("arbitrary", "arbitrary", "arbitrary"),
        cost_estimate=cost(2 * count * rows * depth * width, 2 * count * rows * (depth + width)),
        name="mlp_out",
    )(core[None], *lefts, right)


def weight_grad(lefts, rights, tm, tn):
    _, rows, depth = lefts[0][0].shape
    width = rights[0][0].shape[2]
    count = len(lefts)

    def kernel(*refs):
        total = None
        for c in range(count):
            term = dot(refs[c][0], refs[count + c][0], TN)
            total = term if total is None else total + term
        refs[-1][...] = total

    def left_spec(k):
        return pl.BlockSpec((1, rows, tm), lambda i, j: (k, 0, i))

    def right_spec(k):
        return pl.BlockSpec((1, rows, tn), lambda i, j: (k, 0, j))

    return pl.pallas_call(
        kernel,
        out_shape=jax.ShapeDtypeStruct((depth, width), F32),
        grid=(depth // tm, width // tn),
        in_specs=[left_spec(k) for _, k in lefts] + [right_spec(k) for _, k in rights],
        out_specs=pl.BlockSpec((tm, tn), lambda i, j: (i, j)),
        compiler_params=params("arbitrary", "arbitrary"),
        cost_estimate=cost(2 * count * rows * depth * width, 2 * count * rows * (depth + width)),
        name="weight_grad",
    )(*[a for a, _ in lefts], *[a for a, _ in rights])


def chip_shift(x_in, step, size):
    return lax.ppermute(x_in, "tp", [(t, (t + 2 * step) % size) for t in range(size)])


def swap_cores(x_in, size):
    return lax.ppermute(x_in, "tp", [(t, t ^ 1) for t in range(size)])


def share_weights(pair, me, size):
    chip, core = me // 2, me % 2
    behind, ahead = chip_shift(pair, 1, size), chip_shift(pair, -1, size)
    far = (chip_shift(behind[:1], 1, size), chip_shift(ahead[1:], -1, size))
    near = [(piece, swap_cores(piece, size)) for piece in (pair, behind, ahead)]
    far = [(piece, swap_cores(piece, size)) for piece in far]
    slots = ([], [])
    for pieces in near:
        for piece in pieces:
            slots[0].append((piece, 0))
            slots[1].append((piece, 1))
    for plane in (0, 1):
        slots[plane].extend((piece, 0) for piece in far[plane])
    ranks = []
    for back in (0, -1, 1, 2):
        source = 2 * ((chip + back) % (size // 2))
        ranks += [source + core, source + 1 - core]
    return slots[0], slots[1], jnp.stack(ranks).astype(jnp.int32)


def scatter_by_sends(keep, arrived, chip, size, marks):
    chips, count, shard, depth = keep.shape
    half = shard // 2
    arrived = after(arrived, marks[0])

    def pair_sum(step):
        at = ((chip + step) % chips, 0, 0, 0)
        cut = (1, count, shard, depth)
        return lax.dynamic_slice(keep, at, cut)[0].astype(F32) + lax.dynamic_slice(arrived, at, cut)[0].astype(F32)

    far = pair_sum(2).astype(BF16)
    far_low = after(chip_shift(far[:, :half], 1, size), marks[1])
    far_high = after(chip_shift(far[:, half:], -1, size), marks[1])
    forward, backward = pair_sum(1), pair_sum(-1)
    forward = jnp.concatenate([forward[:, :half] + far_low.astype(F32), forward[:, half:]], axis=1).astype(BF16)
    backward = jnp.concatenate([backward[:, :half], backward[:, half:] + far_high.astype(F32)], axis=1).astype(BF16)
    forward = after(chip_shift(forward, 1, size), marks[2])
    backward = after(chip_shift(backward, -1, size), marks[2])
    return pair_sum(0) + forward.astype(F32) + backward.astype(F32)


def gather(x_loc, axis):
    return lax.all_gather(x_loc, "tp", axis=axis, tiled=True)


def after(value, earlier):
    return lax.optimization_barrier((value, earlier))[0]


def scatter(x_part, axis):
    return lax.psum_scatter(x_part, "tp", scatter_dimension=axis, tiled=True)


def solution(mesh):
    tp_size = mesh.shape["tp"]
    act_spec = P("dp", "tp", None)
    in_specs = (act_spec, act_spec, P("dp"), P("dp"), P(None), P(None, "tp"), P(None, None), P(None, None), P("tp", None), P(None), P(None, "tp"), P(None, "tp"), P("tp", None))
    out_specs = (act_spec, act_spec, P("dp"), P("dp", "tp"), P("dp", None), P("dp", None), P(("dp", "tp"), None), P("dp"), P("dp", "tp"), P("dp", "tp"), P(("dp", "tp"), None))

    def local_layer(hidden, grad_out, prefix_len, valid_len, attn_norm, w_query, w_key, w_value, w_out, mlp_norm, w_gate, w_up, w_down):
        batch, shard_len, model_dim = hidden.shape
        head_dim = w_key.shape[1]
        heads = tp_size * w_query.shape[1] // head_dim
        first = lax.axis_index("tp") * shard_len
        cos_t, sin_t = rope_tables(first + jnp.arange(shard_len), head_dim)
        lens = jnp.concatenate([first[None].astype(jnp.int32), jnp.stack([prefix_len, valid_len], axis=1).reshape(-1).astype(jnp.int32)])

        me = lax.axis_index("tp")
        chip, core = me // 2, me % 2
        wq_slots, wo_slots, ranks = share_weights(jnp.stack([w_query.T, w_out]), me, tp_size)
        normed, norm1_pull = jax.vjp(rms_norm, hidden, attn_norm.astype(F32))
        k_raw = jnp.einsum("bsd,de->bse", normed, w_key, preferred_element_type=F32)
        keys = rotate(k_raw, cos_t, sin_t).astype(BF16)
        values = jnp.einsum("bsd,de->bse", normed, w_value, preferred_element_type=F32).astype(BF16)
        keys_values = gather(jnp.concatenate([keys, values], axis=-1), 1)
        query = rows_to_heads(normed, wq_slots, head_dim, (cos_t, sin_t))
        parts = []
        queue = query
        for start, stop in ((0, 1), (1, batch)):
            mixed, lse = attention_fwd(queue, keys_values, lens, 4, 512, start, stop - start)
            attn_out = heads_to_rows(mixed, wo_slots, model_dim, 1024)
            resid = (hidden[start:stop].astype(F32) + attn_out).astype(BF16)
            gated_in = rms_norm(resid, mlp_norm.astype(F32))
            parts.append((mixed, lse, resid, gated_in))
            queue = after(query, gated_in)
        gated_parts = [parts[0][3]] + [parts[1][3][c:c + 1] for c in range(batch - 1)]
        mixed, lse, resid = (jnp.concatenate([p[i] for p in parts], axis=0) for i in range(3))

        z_all, g_all, acts, d_gates, d_ups, d_gated = [], [], [], [], [], []
        for c in range(batch):
            g_c = (gather(grad_out[c:c + 1], 1), 0)
            z_c = (gather(gated_parts[c], 1), 0)
            if c:
                z_c = (after(z_c[0], d_z_part), 0)
            act, d_gate, d_up = mlp_core(z_c, g_c, w_gate, w_up, w_down, 768, 512)
            d_z_part = product_sum([d_gate, d_up], [w_gate, w_up], NT, BF16, 768, 1024)
            d_gated.append(scatter(d_z_part, 0))
            for items, item in zip((z_all, g_all, acts, d_gates, d_ups), (z_c, g_c, act, d_gate, d_up)):
                items.append(item)

        def planes(arrays):
            return [(a[None], 0) for a in arrays]

        d_resids, norm_parts, dq_parts, d_kv_sums = [], [], [], []
        previous = d_z_part
        for start, stop in ((0, batch - 1), (batch - 1, batch)):
            _, norm2_pull = jax.vjp(rms_norm, resid[start:stop], mlp_norm.astype(F32))
            d_resid_norm, norm_part = norm2_pull(after(jnp.stack(d_gated[start:stop]), previous))
            d_resid = (grad_out[start:stop].astype(F32) + d_resid_norm.astype(F32)).astype(BF16)
            d_mixed = rows_to_heads(d_resid, wo_slots, head_dim)
            dq_part, d_kv_part = attention_bwd(query, keys_values, mixed, d_mixed, lse, cos_t, sin_t, lens, 4, 512, start)
            d_kv_sums.append(scatter(d_kv_part, 1))
            previous = d_kv_part
            d_resids.append(d_resid)
            norm_parts.append(norm_part)
            dq_parts.append(dq_part)
        d_resid = jnp.concatenate(d_resids, axis=0)
        g_mlp_norm_part = norm_parts[0] + norm_parts[1]
        dq_raw = jnp.concatenate(dq_parts, axis=0)
        d_kv = jnp.concatenate(d_kv_sums, axis=0)

        g_query_part = query_weight_grad(after(normed, d_kv_part), dq_raw, ranks)
        g_query = scatter(g_query_part, 0)[0]
        keep, send = split_product(after(acts, g_query_part), w_down, core, tp_size // 2, 768, 1024)
        arrived = swap_cores(send, tp_size)
        d_kv = after(d_kv, keep)
        d_k_raw = rotate(d_kv[..., :head_dim].astype(F32), cos_t, -sin_t).astype(BF16)
        d_kv_raw = jnp.concatenate([d_k_raw, d_kv[..., head_dim:]], axis=-1)
        d_normed = input_grad(dq_raw, d_kv_raw, wq_slots, w_key, w_value, 1024)
        d_hidden_norm, g_attn_norm_part = norm1_pull(d_normed)
        grad_hidden = (d_resid.astype(F32) + d_hidden_norm.astype(F32)).astype(BF16)

        norms = jnp.concatenate([g_attn_norm_part, g_mlp_norm_part]).reshape(-1, 2 * head_dim)
        count = norms.shape[0]
        norms = jnp.pad(norms, ((0, -(model_dim + count) % (8 * heads)), (0, 0)))
        small_part = small_grads(normed, d_kv_raw, norms)
        small = scatter(small_part, 0)
        g_out_part = out_weight_grad(after(mixed, small_part), d_resid, ranks)
        g_out = scatter(g_out_part, 0)

        g_down = weight_grad(planes(after(acts, g_out_part)), g_all, 1024, 512)
        g_gate = weight_grad(z_all, planes(after(d_gates, g_down)), 1024, 512)
        g_up = weight_grad(z_all, planes(after(d_ups, g_gate)), 1024, 512)
        mlp_sum = scatter_by_sends(keep, arrived, chip, tp_size, (small_part, g_down, g_up)).astype(BF16)
        hidden_out = (resid.astype(F32) + mlp_sum.astype(F32)).astype(BF16)
        small = gather(after(small, g_down), 0)
        g_key, g_value = small[:model_dim, :head_dim], small[:model_dim, head_dim:]
        g_norms = small[model_dim:model_dim + count].reshape(2, model_dim)

        return (hidden_out, grad_hidden, g_norms[0], g_query, g_key, g_value, g_out.reshape(-1, model_dim), g_norms[1], g_gate, g_up, g_down)

    return jax.shard_map(local_layer, mesh=mesh, in_specs=in_specs, out_specs=out_specs, check_vma=False)
```
